32 devices in a mesh: gx: 4 (over z), gy: 4 (over y, x), gz: 2 (over core).
Axes of the slice: x: 2, y: 2, z: 4, core: 2. Of those that a mesh axis runs over, the one named last changes fastest.
Arguments:
- metric: float32 [6, 64, 64, 256], P(None, 'gx', 'gy', 'gz'), may hold values from -1 to 9
- curvature: float32 [6, 64, 64, 256], P(None, 'gx', 'gy', 'gz'), may hold values from -1.8 to 1.8
- conserved: float32 [4, 64, 64, 256], P(None, 'gx', 'gy', 'gz'), may hold values from -0.3 to 1, as said below
- matter_mask: int32 [4, 4, 16], P('gx', 'gy', 'gz'), may hold values from 0 to 1, as said below
Outputs:
- metric_next: float32 [6, 64, 64, 256], P(None, 'gx', 'gy', 'gz')
- curvature_next: float32 [6, 64, 64, 256], P(None, 'gx', 'gy', 'gz')
- conserved_next: float32 [4, 64, 64, 256], P(None, 'gx', 'gy', 'gz')
The draws below stay inside these ranges and needn't reach their ends.
Inputs may be any that keep to these rules, and one draw needn't show every extreme that they name: `conserved`: component 0 is the density, from 0.25 to 1; components 1 to 3 are the momentum. `matter_mask`: 1 marks a matter-bearing meshblock of 16 x 16 x 16 cells.
All inputs are finite; a program needn't handle non-finite values.
Results may differ from the reference program's by a relative error of at most 0.00002.
Values sent between devices are 32-bit elements; how exact they have to be, the bound alone decides.
A program may use at most 64 MiB of HBM per device.

```python
import math
import jax
import jax.numpy as jnp

MB = 16
NX = 64
NY = 64
NZ = 256
KX = 4
KY = 4
KZ = 16


def draw_metric(key, part):
    key_phase = jax.random.fold_in(key, 31)
    key_rough = jax.random.fold_in(key, 32)
    phases = jax.random.uniform(key_phase, (6, 3), jnp.float32, 0.0, 2.0 * jnp.pi)
    coord_x = 2.0 * jnp.pi / NX * jnp.arange(NX, dtype=jnp.float32)
    coord_y = 2.0 * jnp.pi / NY * jnp.arange(NY, dtype=jnp.float32)
    coord_z = 2.0 * jnp.pi / NZ * jnp.arange(NZ, dtype=jnp.float32)
    wave_x = jnp.cos(coord_x[None, :] + phases[:, 0:1])[:, :, None, None]
    wave_y = jnp.cos(coord_y[None, :] + phases[:, 1:2])[:, None, :, None]
    wave_z = jnp.cos(coord_z[None, :] + phases[:, 2:3])[:, None, None, :]
    smooth = 1.5 * wave_x * wave_y * wave_z
    rough = jnp.clip(jax.random.normal(key_rough, (6, NX, NY, NZ), jnp.float32), -3.0, 3.0)
    return 4.0 + smooth + rough


def draw_conserved(key, part):
    key_density = jax.random.fold_in(key, 11)
    key_moment = jax.random.fold_in(key, 12)
    position = jnp.arange(NX, dtype=jnp.float32) / max(NX - 1, 1)
    density = jnp.exp(jax.random.uniform(key_density, (1, NX, NY, NZ), jnp.float32, jnp.log(0.25), jnp.log(1.0)))
    rising = (0.03 * (1.0 + 2.0 * position))[None, :, None, None]
    moment = jnp.clip(jax.random.normal(key_moment, (3, NX, NY, NZ), jnp.float32), -3.0, 3.0) * rising
    return jnp.concatenate([density, moment], axis=0)


def draw_matter_mask(key, part):
    index_x = jnp.arange(KX, dtype=jnp.int32)[:, None, None]
    index_y = jnp.arange(KY, dtype=jnp.int32)[None, :, None]
    index_z = jnp.arange(KZ, dtype=jnp.int32)[None, None, :]
    offset_x = 2 * index_x + 1 - KX
    offset_y = 2 * index_y + 1 - KY
    offset_z = 2 * index_z + 1 - KZ
    radius = offset_x * offset_x * 100 // (KX * KX) + offset_y * offset_y * 100 // (KY * KY) + offset_z * offset_z * 100 // (KZ * KZ)
    threshold = jnp.maximum(700 - 5 * radius, 30)
    sample = jax.random.randint(jax.random.fold_in(key, 21), (KX, KY, KZ), 0, 1000)
    return (sample < threshold).astype(jnp.int32)


def shard_levels(stream_key, shape, cuts, smallest, top_value):
    factor_of = 1.0
    for dim, parts in cuts:
        draws = jax.random.uniform(jax.random.fold_in(jax.random.fold_in(stream_key, 6), dim), (parts,), jnp.float32, smallest / len(cuts), top_value / len(cuts))
        factor_of = factor_of * jnp.repeat(jnp.exp(draws), shape[dim] // parts).reshape((-1,) + (1,) * (len(shape) - 1 - dim))
    return factor_of


def bell_draw(stream_key, extent, deviation, bound, split=(), held_as=jnp.bfloat16):
    array = deviation * jax.random.normal(stream_key, extent, jnp.float32)
    if split:
        array = array * shard_levels(stream_key, extent, split, -0.22, 0.18)
    return jnp.clip(array, -bound, bound).astype(held_as)


def setup_inputs(seed: int = 0) -> dict:
    arg_keys = jax.random.split(jax.random.key(seed), 5)
    metric = draw_metric(jax.random.fold_in(arg_keys[4], 71), 0)
    curvature = bell_draw(arg_keys[1], (6, NX, NY, NZ), 0.3, 1.8, ((1, 4), (2, 4), (3, 2)), jnp.float32)
    conserved = draw_conserved(jax.random.fold_in(arg_keys[4], 71), 0)
    matter_mask = draw_matter_mask(jax.random.fold_in(arg_keys[4], 71), 0)
    return dict(metric=metric, curvature=curvature, conserved=conserved, matter_mask=matter_mask)


second_stencil = (1.0 / 90.0, -3.0 / 20.0, 1.5, -49.0 / 18.0, 1.5, -3.0 / 20.0, 1.0 / 90.0)
first_stencil = (-1.0 / 60.0, 3.0 / 20.0, -0.75, 0.0, 0.75, -3.0 / 20.0, 1.0 / 60.0)
sound_square = 0.25
sound_speed = 0.5
courant = 0.3
eight_pi = 8.0 * math.pi
pair_first = (0, 0, 0, 1, 1, 2)
pair_second = (0, 1, 2, 1, 2, 2)


def expand_mask(matter_mask, block_edge):
    blocks_x, blocks_y, blocks_z = matter_mask.shape
    spread = jnp.broadcast_to(matter_mask[:, None, :, None, :, None], (blocks_x, block_edge, blocks_y, block_edge, blocks_z, block_edge))
    return spread.reshape(blocks_x * block_edge, blocks_y * block_edge, blocks_z * block_edge) > 0


def rolled_sum(field, stencil, axis_index):
    total = jnp.zeros_like(field)
    for offset in range(-3, 4):
        if stencil[offset + 3] != 0.0:
            total = total + stencil[offset + 3] * jnp.roll(field, -offset, axis=axis_index)
    return total


def reference(metric, curvature, conserved, matter_mask):
    cell_mask = expand_mask(matter_mask, MB)
    density = conserved[0]
    moment = conserved[1:4]
    speed = jnp.max(jnp.abs(moment), axis=0) / density + sound_speed
    speed_max = jnp.max(jnp.where(cell_mask, speed, jnp.float32(sound_speed)))
    step = courant / speed_max
    laplacian = rolled_sum(metric, second_stencil, 1)
    laplacian = laplacian + rolled_sum(metric, second_stencil, 2)
    laplacian = laplacian + rolled_sum(metric, second_stencil, 3)
    stress_list = []
    for component in range(6):
        first = pair_first[component]
        second = pair_second[component]
        term = moment[first] * moment[second] / density
        if first == second:
            term = term + sound_square * density
        stress_list.append(term)
    stress = jnp.stack(stress_list)
    curvature_next = curvature + step * (eight_pi * stress - 0.5 * laplacian)
    metric_next = metric - 2.0 * step * curvature
    potential = 0.5 * (metric[0] + metric[3] + metric[5])
    gradient = jnp.stack([rolled_sum(potential, first_stencil, direction) for direction in range(3)])
    divergence = jnp.zeros_like(conserved)
    for direction in range(3):
        velocity = moment[direction] / density
        flux_moment = moment * velocity[None]
        flux_moment = flux_moment.at[direction].add(sound_square * density)
        flux = jnp.concatenate([moment[direction][None], flux_moment], axis=0)
        upper_flux = jnp.roll(flux, -1, axis=direction + 1)
        upper_state = jnp.roll(conserved, -1, axis=direction + 1)
        face = 0.5 * (flux + upper_flux) - 0.5 * speed_max * (upper_state - conserved)
        divergence = divergence + (face - jnp.roll(face, 1, axis=direction + 1))
    source = jnp.concatenate([jnp.zeros_like(density)[None], density[None] * gradient], axis=0)
    advanced = conserved - step * divergence + step * source
    conserved_next = jnp.where(cell_mask[None], advanced, conserved)
    return metric_next, curvature_next, conserved_next
```

```python
import functools
import math

import jax
import jax.numpy as jnp
from jax import lax
from jax.experimental import pallas as pl
from jax.experimental.pallas import tpu as pltpu
from jax.sharding import PartitionSpec as P

MESH = pl.DeviceIdType.MESH
AXES = ("gx", "gy", "gz")
MB = 16
second = (-49.0 / 18.0, 1.5, -3.0 / 20.0, 1.0 / 90.0)
first = (0.0, 0.75, -3.0 / 20.0, 1.0 / 60.0)
sound_square = 0.25
sound_speed = 0.5
courant = 0.3
eight_pi = 8.0 * math.pi
pair_first = (0, 0, 0, 1, 1, 2)
pair_second = (0, 1, 2, 1, 2, 2)
trace_part = (0, 3, 5)
W = 3
SUB = 8


def peer(sizes, axes, offset):
    position = 0
    for axis in axes:
        position = position * sizes[axis] + lax.axis_index(axis)
    total = math.prod(sizes[axis] for axis in axes)
    position = lax.rem(position + offset, total)
    found = {}
    for axis in reversed(axes):
        found[axis] = lax.rem(position, sizes[axis])
        position = position // sizes[axis]
    return {axis: found.get(axis, lax.axis_index(axis)) for axis in AXES}


def stages_of(sizes):
    if math.prod(sizes.values()) <= 64:
        return (AXES,)
    return (("gz",), ("gy",), ("gx",))


def flux_of(state, direction):
    density, moment = state[0], state[1:]
    velocity = moment[direction] / density
    flux = [moment[direction]] + [moment[i] * velocity for i in range(3)]
    flux[1 + direction] = flux[1 + direction] + sound_square * density
    return flux


def kernel(sizes, shape, metric_hbm, fluid_hbm, mask_ref, curv_out, fluid_out, step_out,
           mp, up, ez, uz, ey, uy, acc_c, acc_f, acc_l, row, *rest):
    nx, ny, nz = shape
    stages = stages_of(sizes)
    bufs = rest[: len(stages)]
    load_sem, send_sem, recv_sem, row_send, row_recv = rest[len(stages):]
    tiles = ny // SUB

    own_m = mp.at[:, pl.ds(W, nx)]
    own_u = up.at[:, pl.ds(1, nx)]
    load_u = pltpu.make_async_copy(fluid_hbm, own_u, load_sem.at[0])
    load_m = pltpu.make_async_copy(metric_hbm, own_m, load_sem.at[1])
    load_u.start()
    load_m.start()

    barrier = pltpu.get_barrier_semaphore()
    greeted = 0
    for axes in stages:
        total = math.prod(sizes[axis] for axis in axes)

        def greet(j, carry, axes=axes):
            pl.semaphore_signal(barrier, inc=1, device_id=peer(sizes, axes, j), device_id_type=MESH)
            return carry

        lax.fori_loop(1, total, greet, 0)
        greeted += total - 1

    lane = lax.broadcasted_iota(jnp.int32, (ny, nz), 1)
    block = lane // MB
    mask = jnp.zeros((ny, nz), jnp.int32)
    for b in range(nz // MB):
        mask = jnp.where(block == b, mask_ref[0, 0, b], mask)
    mask = mask > 0

    load_u.wait()

    def local_speed(x, best):
        moment = jnp.maximum(jnp.maximum(jnp.abs(up[1, x + 1]), jnp.abs(up[2, x + 1])), jnp.abs(up[3, x + 1]))
        speed = moment / up[0, x + 1] + sound_speed
        return jnp.maximum(best, jnp.where(mask, speed, jnp.float32(sound_speed)))

    best = lax.fori_loop(0, nx, local_speed, jnp.full((ny, nz), sound_speed, jnp.float32), unroll=4)
    best = jnp.max(best, axis=0, keepdims=True)
    row[0] = best
    load_m.wait()
    pl.semaphore_wait(barrier, greeted)

    def spread(index):
        axes = stages[index]
        total = math.prod(sizes[axis] for axis in axes)

        def send(j, carry):
            pltpu.make_async_remote_copy(
                src_ref=row.at[index], dst_ref=bufs[index].at[j - 1],
                send_sem=row_send.at[index], recv_sem=row_recv.at[index],
                device_id=peer(sizes, axes, j), device_id_type=MESH,
            ).start()
            return carry

        lax.fori_loop(1, total, send, 0)

    def gathered(index, best):
        buf = bufs[index]
        pltpu.make_async_copy(buf, buf, row_recv.at[index]).wait()
        pltpu.make_async_copy(buf, buf, row_send.at[index]).wait()
        return jnp.maximum(best, jnp.max(buf[...], axis=0))

    spread(0)

    count = [0]

    def remote(src, dst, axis, offset):
        n = count[0]
        count[0] += 1
        copy = pltpu.make_async_remote_copy(
            src_ref=src, dst_ref=dst, send_sem=send_sem.at[n], recv_sem=recv_sem.at[n],
            device_id=peer(sizes, (axis,), offset % sizes[axis]), device_id_type=MESH,
        )
        copy.start()
        return copy

    y_copies = [
        remote(mp.at[:, pl.ds(W, nx), pl.ds(ny - W, W)], ey.at[:, :, pl.ds(SUB - W, W)], "gy", 1),
        remote(mp.at[:, pl.ds(W, nx), pl.ds(0, W)], ey.at[:, :, pl.ds(0, W)], "gy", -1),
        remote(up.at[:, pl.ds(1, nx), pl.ds(ny - 1, 1)], uy.at[:, :, pl.ds(SUB - 1, 1)], "gy", 1),
        remote(up.at[:, pl.ds(1, nx), pl.ds(0, 1)], uy.at[:, :, pl.ds(0, 1)], "gy", -1),
    ]
    x_copies = [
        remote(mp.at[:, pl.ds(nx, W)], mp.at[:, pl.ds(0, W)], "gx", 1),
        remote(mp.at[:, pl.ds(W, W)], mp.at[:, pl.ds(nx + W, W)], "gx", -1),
        remote(up.at[:, pl.ds(nx, 1)], up.at[:, pl.ds(0, 1)], "gx", 1),
        remote(up.at[:, pl.ds(1, 1)], up.at[:, pl.ds(nx + 1, 1)], "gx", -1),
    ]
    z_copies = [remote(own_u, uz.at[0], "gz", -1), remote(own_m, ez.at[0], "gz", -1)]
    if sizes["gz"] > 2:
        z_copies += [remote(own_u, uz.at[1], "gz", 1), remote(own_m, ez.at[1], "gz", 1)]

    def edge(ref, c, x):
        if sizes["gz"] > 2:
            return jnp.where(lane < nz // 2, ref[0, c, x], ref[1, c, x])
        return ref[0, c, x]

    def z_up(own, other, k):
        return pltpu.roll(jnp.where(lane < k, other, own), nz - k, 1)

    def z_down(own, other, k):
        return pltpu.roll(jnp.where(lane >= nz - k, other, own), k, 1)

    sub = lax.broadcasted_iota(jnp.int32, (SUB, nz), 0)

    def cut(value):
        return [value[t * SUB : (t + 1) * SUB] for t in range(tiles)]

    def y_pair(value, k):
        own = cut(value)
        zero = jnp.zeros_like(own[0])
        after = own[1:] + [zero]
        before = [zero] + own[:-1]
        up_rows = [pltpu.roll(jnp.where(sub < k, after[t], own[t]), SUB - k, 0) for t in range(tiles)]
        down_rows = [pltpu.roll(jnp.where(sub >= SUB - k, before[t], own[t]), k, 0) for t in range(tiles)]
        return jnp.concatenate(up_rows, axis=0), jnp.concatenate(down_rows, axis=0)

    for copy in z_copies:
        copy.wait()

    def inner(x, carry):
        state = [up[c, x + 1] for c in range(4)]
        density, moment = state[0], state[1:]
        other = [edge(uz, c, x) for c in range(4)]
        above = [z_up(state[c], other[c], 1) for c in range(4)]
        below = [z_down(state[c], other[c], 1) for c in range(4)]
        flux_above, flux_below = flux_of(above, 2), flux_of(below, 2)
        flux_y = flux_of(state, 1)
        slopes = []
        for c in range(4):
            y_above, y_below = y_pair(state[c], 1)
            fy_above, fy_below = y_pair(flux_y[c], 1)
            slopes.append((flux_above[c] - flux_below[c]) + (fy_above - fy_below))
            acc_l[c, x] = (above[c] + below[c]) + (y_above + y_below) - 6.0 * state[c]
        grad_y = jnp.zeros((ny, nz), jnp.float32)
        grad_z = jnp.zeros((ny, nz), jnp.float32)
        inverse = 1.0 / density
        for c in range(6):
            own = mp[c, x + W]
            far = edge(ez, c, x)
            total = (3.0 * second[0]) * own
            for k in range(1, W + 1):
                zu, zd = z_up(own, far, k), z_down(own, far, k)
                yu, yd = y_pair(own, k)
                total = total + second[k] * ((zu + zd) + (yu + yd))
                if c in trace_part:
                    grad_z = grad_z + first[k] * (zu - zd)
                    grad_y = grad_y + first[k] * (yu - yd)
            stress = moment[pair_first[c]] * (moment[pair_second[c]] * inverse)
            if pair_first[c] == pair_second[c]:
                stress = stress + sound_square * density
            acc_c[c, x] = eight_pi * stress - 0.5 * total
        acc_f[0, x] = -0.5 * slopes[0]
        acc_f[1, x] = -0.5 * slopes[1]
        acc_f[2, x] = -0.5 * slopes[2] + (0.5 * density) * grad_y
        acc_f[3, x] = -0.5 * slopes[3] + (0.5 * density) * grad_z
        return carry

    lax.fori_loop(0, nx, inner, 0)

    for copy in x_copies:
        copy.wait()

    def along_x(x, carry):
        above = [up[c, x + 2] for c in range(4)]
        below = [up[c, x] for c in range(4)]
        flux_above, flux_below = flux_of(above, 0), flux_of(below, 0)
        grad = jnp.zeros((ny, nz), jnp.float32)
        for c in range(6):
            total = jnp.zeros((ny, nz), jnp.float32)
            for k in range(1, W + 1):
                high, low = mp[c, x + W + k], mp[c, x + W - k]
                total = total + second[k] * (high + low)
                if c in trace_part:
                    grad = grad + first[k] * (high - low)
            acc_c[c, x] = acc_c[c, x] - 0.5 * total
        for c in range(4):
            value = acc_f[c, x] - 0.5 * (flux_above[c] - flux_below[c])
            if c == 1:
                value = value + (0.5 * up[0, x + 1]) * grad
            acc_f[c, x] = value
            acc_l[c, x] = acc_l[c, x] + (above[c] + below[c])
        return carry

    lax.fori_loop(0, nx, along_x, 0)

    best = gathered(0, best)
    for index in range(1, len(stages)):
        row[index] = best
        spread(index)
        best = gathered(index, best)
    speed_max = jnp.max(best, axis=1, keepdims=True)
    step = courant / speed_max
    step_out[...] = jnp.broadcast_to(step, step_out.shape)
    step_all = jnp.broadcast_to(step, (ny, nz))
    half_speed = jnp.broadcast_to(0.5 * speed_max, (ny, nz))

    for copy in y_copies:
        copy.wait()

    inside = jnp.logical_and(sub >= W, sub < SUB - W)
    weight, slope = [None], [None]
    for k in range(1, W + 1):
        touched = jnp.where(jnp.logical_or(sub < k, sub >= SUB - k), 1.0, 0.0)
        weight.append(touched * jnp.float32(second[k]))
        slope.append(jnp.where(sub < SUB // 2, -1.0, 1.0) * touched * jnp.float32(first[k]))
    low_half = sub < SUB // 2
    nothing = jnp.zeros((SUB, nz), jnp.float32)

    def placed(value):
        parts = [jnp.where(low_half, value, nothing)] + [nothing] * (tiles - 2) + [jnp.where(low_half, nothing, value)]
        return jnp.concatenate(parts, axis=0)

    def finish(x, carry):
        grad = nothing
        for c in range(6):
            halo = jnp.where(inside, nothing, ey[c, x])
            total = nothing
            for k in range(1, W + 1):
                near = jnp.where(low_half, pltpu.roll(halo, k, 0), pltpu.roll(halo, SUB - k, 0))
                total = total + weight[k] * near
                if c in trace_part:
                    grad = grad + slope[k] * near
            curv_out[c, x] = step_all * (acc_c[c, x] - 0.5 * placed(total))
        halo = [uy[c, x] for c in range(4)]
        flux = flux_of(halo, 1)
        density = up[0, x + 1]
        for c in range(4):
            near = jnp.where(sub == 0, pltpu.roll(halo[c], 1, 0), pltpu.roll(halo[c], SUB - 1, 0))
            near_flux = jnp.where(sub == 0, -pltpu.roll(flux[c], 1, 0), pltpu.roll(flux[c], SUB - 1, 0))
            end = jnp.logical_or(sub == 0, sub == SUB - 1)
            near = placed(jnp.where(end, near, nothing))
            near_flux = placed(jnp.where(end, near_flux, nothing))
            value = acc_f[c, x] - 0.5 * near_flux
            if c == 2:
                value = value + (0.5 * density) * placed(grad)
            value = step_all * (value + half_speed * (acc_l[c, x] + near))
            fluid_out[c, x] = jnp.where(mask, value, 0.0)
        return carry

    lax.fori_loop(0, nx, finish, 0)


def body(sizes, metric, curvature, conserved, matter_mask):
    shape = metric.shape[1:]
    nx, ny, nz = shape
    assert matter_mask.shape[:2] == (1, 1) and ny % SUB == 0 and ny >= 2 * SUB
    stages = stages_of(sizes)
    totals = [math.prod(sizes[axis] for axis in axes) for axes in stages]
    sides = 2 if sizes["gz"] > 2 else 1
    copies = 8 + 2 * sides
    vmem, sem = pltpu.VMEM, pltpu.SemaphoreType.DMA
    f32 = jnp.float32
    curv_add, fluid_add, step = pl.pallas_call(
        functools.partial(kernel, sizes, shape),
        out_shape=(
            jax.ShapeDtypeStruct((6,) + shape, f32),
            jax.ShapeDtypeStruct((4,) + shape, f32),
            jax.ShapeDtypeStruct((SUB, nz), f32),
        ),
        in_specs=[
            pl.BlockSpec(memory_space=pl.ANY),
            pl.BlockSpec(memory_space=pl.ANY),
            pl.BlockSpec(memory_space=pltpu.SMEM),
        ],
        out_specs=(pl.BlockSpec(memory_space=vmem),) * 3,
        scratch_shapes=[
            vmem((6, nx + 2 * W, ny, nz), f32),
            vmem((4, nx + 2, ny, nz), f32),
            vmem((sides, 6, nx, ny, nz), f32),
            vmem((sides, 4, nx, ny, nz), f32),
            vmem((6, nx, SUB, nz), f32),
            vmem((4, nx, SUB, nz), f32),
            vmem((6, nx, ny, nz), f32),
            vmem((4, nx, ny, nz), f32),
            vmem((4, nx, ny, nz), f32),
            vmem((len(stages), 1, nz), f32),
        ]
        + [vmem((total - 1, 1, nz), f32) for total in totals]
        + [sem((2,)), sem((copies,)), sem((copies,)), sem((len(stages),)), sem((len(stages),))],
        compiler_params=pltpu.CompilerParams(
            collective_id=0, has_side_effects=True, vmem_limit_bytes=24 * 1024 * 1024
        ),
        name="substep",
    )(metric, conserved, matter_mask)
    metric_next = metric - (2.0 * step[0, 0]) * curvature
    return metric_next, curvature + curv_add, conserved + fluid_add


def solution(mesh):
    sizes = {axis: mesh.shape[axis] for axis in AXES}
    grid = P(None, "gx", "gy", "gz")
    return jax.shard_map(
        functools.partial(body, sizes),
        mesh=mesh,
        in_specs=(grid, grid, grid, P("gx", "gy", "gz")),
        out_specs=(grid, grid, grid),
        check_vma=False,
    )
```

```python
import functools
import math

import jax
import jax.numpy as jnp
from jax import lax
from jax.experimental import pallas as pl
from jax.experimental.pallas import tpu as pltpu
from jax.sharding import PartitionSpec as P

MESH = pl.DeviceIdType.MESH
AXES = ("gx", "gy", "gz")
MB = 16
second = (-49.0 / 18.0, 1.5, -3.0 / 20.0, 1.0 / 90.0)
first = (0.0, 0.75, -3.0 / 20.0, 1.0 / 60.0)
sound_square = 0.25
sound_speed = 0.5
courant = 0.3
eight_pi = 8.0 * math.pi
pair_first = (0, 0, 0, 1, 1, 2)
pair_second = (0, 1, 2, 1, 2, 2)
trace_part = (0, 3, 5)
W = 3
SUB = 8


def peer(sizes, axes, offset):
    position = 0
    for axis in axes:
        position = position * sizes[axis] + lax.axis_index(axis)
    total = math.prod(sizes[axis] for axis in axes)
    position = lax.rem(position + offset, total)
    found = {}
    for axis in reversed(axes):
        found[axis] = lax.rem(position, sizes[axis])
        position = position // sizes[axis]
    return {axis: found.get(axis, lax.axis_index(axis)) for axis in AXES}


def stages_of(sizes):
    if math.prod(sizes.values()) <= 64:
        return (AXES,)
    return (("gz",), ("gy",), ("gx",))


def flux_of(state, direction):
    density, moment = state[0], state[1:]
    velocity = moment[direction] / density
    flux = [moment[direction]] + [moment[i] * velocity for i in range(3)]
    flux[1 + direction] = flux[1 + direction] + sound_square * density
    return flux


def kernel(sizes, shape, metric_hbm, curv_hbm, fluid_hbm, mask_hbm, metric_out, curv_out, fluid_out,
           mask_ref, cu, mp, up, ez, uz, ey, uy, acc_c, acc_f, acc_l, row, *rest):
    nx, ny, nz = shape
    stages = stages_of(sizes)
    bufs = rest[: len(stages)]
    load_sem, send_sem, recv_sem, row_send, row_recv = rest[len(stages):]
    tiles = ny // SUB

    own_m = mp.at[:, pl.ds(W, nx)]
    own_u = up.at[:, pl.ds(1, nx)]
    load_u = pltpu.make_async_copy(fluid_hbm, own_u, load_sem.at[0])
    load_m = pltpu.make_async_copy(metric_hbm, own_m, load_sem.at[1])
    load_mask = pltpu.make_async_copy(mask_hbm, mask_ref, load_sem.at[2])
    load_c = pltpu.make_async_copy(curv_hbm, cu, load_sem.at[3])
    load_mask.start()
    load_u.start()
    load_m.start()
    load_c.start()

    barrier = pltpu.get_barrier_semaphore()
    greeted = 0
    for axes in stages:
        total = math.prod(sizes[axis] for axis in axes)

        def greet(j, carry, axes=axes):
            pl.semaphore_signal(barrier, inc=1, device_id=peer(sizes, axes, j), device_id_type=MESH)
            return carry

        lax.fori_loop(1, total, greet, 0)
        greeted += total - 1

    load_mask.wait()
    lane = lax.broadcasted_iota(jnp.int32, (ny, nz), 1)
    block = lane // MB
    mask = jnp.zeros((ny, nz), jnp.int32)
    for b in range(nz // MB):
        mask = jnp.where(block == b, mask_ref[0, 0, b], mask)
    mask = mask > 0

    load_u.wait()

    def local_speed(x, best):
        moment = jnp.maximum(jnp.maximum(jnp.abs(up[1, x + 1]), jnp.abs(up[2, x + 1])), jnp.abs(up[3, x + 1]))
        speed = moment / up[0, x + 1] + sound_speed
        return jnp.maximum(best, jnp.where(mask, speed, jnp.float32(sound_speed)))

    best = lax.fori_loop(0, nx, local_speed, jnp.full((ny, nz), sound_speed, jnp.float32), unroll=4)
    best = jnp.max(best, axis=0, keepdims=True)
    row[0] = best
    load_m.wait()
    pl.semaphore_wait(barrier, greeted)

    def spread(index):
        axes = stages[index]
        total = math.prod(sizes[axis] for axis in axes)

        def send(j, carry):
            pltpu.make_async_remote_copy(
                src_ref=row.at[index], dst_ref=bufs[index].at[j - 1],
                send_sem=row_send.at[index], recv_sem=row_recv.at[index],
                device_id=peer(sizes, axes, j), device_id_type=MESH,
            ).start()
            return carry

        lax.fori_loop(1, total, send, 0)

    def gathered(index, best):
        buf = bufs[index]
        pltpu.make_async_copy(buf, buf, row_recv.at[index]).wait()
        pltpu.make_async_copy(buf, buf, row_send.at[index]).wait()
        return jnp.maximum(best, jnp.max(buf[...], axis=0))

    spread(0)

    count = [0]

    def remote(src, dst, axis, offset):
        n = count[0]
        count[0] += 1
        copy = pltpu.make_async_remote_copy(
            src_ref=src, dst_ref=dst, send_sem=send_sem.at[n], recv_sem=recv_sem.at[n],
            device_id=peer(sizes, (axis,), offset % sizes[axis]), device_id_type=MESH,
        )
        copy.start()
        return copy

    y_copies = [
        remote(mp.at[:, pl.ds(W, nx), pl.ds(ny - W, W)], ey.at[:, :, pl.ds(SUB - W, W)], "gy", 1),
        remote(mp.at[:, pl.ds(W, nx), pl.ds(0, W)], ey.at[:, :, pl.ds(0, W)], "gy", -1),
        remote(up.at[:, pl.ds(1, nx), pl.ds(ny - 1, 1)], uy.at[:, :, pl.ds(SUB - 1, 1)], "gy", 1),
        remote(up.at[:, pl.ds(1, nx), pl.ds(0, 1)], uy.at[:, :, pl.ds(0, 1)], "gy", -1),
    ]
    x_copies = [
        remote(mp.at[:, pl.ds(nx, W)], mp.at[:, pl.ds(0, W)], "gx", 1),
        remote(mp.at[:, pl.ds(W, W)], mp.at[:, pl.ds(nx + W, W)], "gx", -1),
        remote(up.at[:, pl.ds(nx, 1)], up.at[:, pl.ds(0, 1)], "gx", 1),
        remote(up.at[:, pl.ds(1, 1)], up.at[:, pl.ds(nx + 1, 1)], "gx", -1),
    ]
    z_copies = [remote(own_u, uz.at[0], "gz", -1), remote(own_m, ez.at[0], "gz", -1)]
    if sizes["gz"] > 2:
        z_copies += [remote(own_u, uz.at[1], "gz", 1), remote(own_m, ez.at[1], "gz", 1)]

    def edge(ref, c, x):
        if sizes["gz"] > 2:
            return jnp.where(lane < nz // 2, ref[0, c, x], ref[1, c, x])
        return ref[0, c, x]

    def z_up(own, other, k):
        return pltpu.roll(jnp.where(lane < k, other, own), nz - k, 1)

    def z_down(own, other, k):
        return pltpu.roll(jnp.where(lane >= nz - k, other, own), k, 1)

    sub = lax.broadcasted_iota(jnp.int32, (SUB, nz), 0)

    def cut(value):
        return [value[t * SUB : (t + 1) * SUB] for t in range(tiles)]

    def y_pair(value, k):
        own = cut(value)
        zero = jnp.zeros_like(own[0])
        after = own[1:] + [zero]
        before = [zero] + own[:-1]
        up_rows = [pltpu.roll(jnp.where(sub < k, after[t], own[t]), SUB - k, 0) for t in range(tiles)]
        down_rows = [pltpu.roll(jnp.where(sub >= SUB - k, before[t], own[t]), k, 0) for t in range(tiles)]
        return jnp.concatenate(up_rows, axis=0), jnp.concatenate(down_rows, axis=0)

    for copy in z_copies:
        copy.wait()

    def inner(x, carry):
        state = [up[c, x + 1] for c in range(4)]
        density, moment = state[0], state[1:]
        other = [edge(uz, c, x) for c in range(4)]
        above = [z_up(state[c], other[c], 1) for c in range(4)]
        below = [z_down(state[c], other[c], 1) for c in range(4)]
        flux_above, flux_below = flux_of(above, 2), flux_of(below, 2)
        flux_y = flux_of(state, 1)
        slopes = []
        for c in range(4):
            y_above, y_below = y_pair(state[c], 1)
            fy_above, fy_below = y_pair(flux_y[c], 1)
            slopes.append((flux_above[c] - flux_below[c]) + (fy_above - fy_below))
            acc_l[c, x] = (above[c] + below[c]) + (y_above + y_below) - 6.0 * state[c]
        grad_y = jnp.zeros((ny, nz), jnp.float32)
        grad_z = jnp.zeros((ny, nz), jnp.float32)
        inverse = 1.0 / density
        for c in range(6):
            own = mp[c, x + W]
            far = edge(ez, c, x)
            total = (3.0 * second[0]) * own
            for k in range(1, W + 1):
                zu, zd = z_up(own, far, k), z_down(own, far, k)
                yu, yd = y_pair(own, k)
                total = total + second[k] * ((zu + zd) + (yu + yd))
                if c in trace_part:
                    grad_z = grad_z + first[k] * (zu - zd)
                    grad_y = grad_y + first[k] * (yu - yd)
            stress = moment[pair_first[c]] * (moment[pair_second[c]] * inverse)
            if pair_first[c] == pair_second[c]:
                stress = stress + sound_square * density
            acc_c[c, x] = eight_pi * stress - 0.5 * total
        acc_f[0, x] = -0.5 * slopes[0]
        acc_f[1, x] = -0.5 * slopes[1]
        acc_f[2, x] = -0.5 * slopes[2] + (0.5 * density) * grad_y
        acc_f[3, x] = -0.5 * slopes[3] + (0.5 * density) * grad_z
        return carry

    lax.fori_loop(0, nx, inner, 0)

    for copy in x_copies:
        copy.wait()

    def along_x(x, carry):
        above = [up[c, x + 2] for c in range(4)]
        below = [up[c, x] for c in range(4)]
        flux_above, flux_below = flux_of(above, 0), flux_of(below, 0)
        grad = jnp.zeros((ny, nz), jnp.float32)
        for c in range(6):
            total = jnp.zeros((ny, nz), jnp.float32)
            for k in range(1, W + 1):
                high, low = mp[c, x + W + k], mp[c, x + W - k]
                total = total + second[k] * (high + low)
                if c in trace_part:
                    grad = grad + first[k] * (high - low)
            acc_c[c, x] = acc_c[c, x] - 0.5 * total
        for c in range(4):
            value = acc_f[c, x] - 0.5 * (flux_above[c] - flux_below[c])
            if c == 1:
                value = value + (0.5 * up[0, x + 1]) * grad
            acc_f[c, x] = value
            acc_l[c, x] = acc_l[c, x] + (above[c] + below[c])
        return carry

    lax.fori_loop(0, nx, along_x, 0)

    best = gathered(0, best)
    for index in range(1, len(stages)):
        row[index] = best
        spread(index)
        best = gathered(index, best)
    speed_max = jnp.max(best, axis=1, keepdims=True)
    step = courant / speed_max
    step_all = jnp.broadcast_to(step, (ny, nz))
    half_speed = jnp.broadcast_to(0.5 * speed_max, (ny, nz))

    load_c.wait()

    def advance_metric(x, carry):
        for c in range(6):
            metric_out[c, x] = mp[c, x + W] - (2.0 * step_all) * cu[c, x]
        return carry

    lax.fori_loop(0, nx, advance_metric, 0)

    for copy in y_copies:
        copy.wait()

    inside = jnp.logical_and(sub >= W, sub < SUB - W)
    weight, slope = [None], [None]
    for k in range(1, W + 1):
        touched = jnp.where(jnp.logical_or(sub < k, sub >= SUB - k), 1.0, 0.0)
        weight.append(touched * jnp.float32(second[k]))
        slope.append(jnp.where(sub < SUB // 2, -1.0, 1.0) * touched * jnp.float32(first[k]))
    low_half = sub < SUB // 2
    nothing = jnp.zeros((SUB, nz), jnp.float32)

    def placed(value):
        parts = [jnp.where(low_half, value, nothing)] + [nothing] * (tiles - 2) + [jnp.where(low_half, nothing, value)]
        return jnp.concatenate(parts, axis=0)

    def finish(x, carry):
        grad = nothing
        for c in range(6):
            halo = jnp.where(inside, nothing, ey[c, x])
            total = nothing
            for k in range(1, W + 1):
                near = jnp.where(low_half, pltpu.roll(halo, k, 0), pltpu.roll(halo, SUB - k, 0))
                total = total + weight[k] * near
                if c in trace_part:
                    grad = grad + slope[k] * near
            curv_out[c, x] = cu[c, x] + step_all * (acc_c[c, x] - 0.5 * placed(total))
        halo = [uy[c, x] for c in range(4)]
        flux = flux_of(halo, 1)
        density = up[0, x + 1]
        for c in range(4):
            near = jnp.where(sub == 0, pltpu.roll(halo[c], 1, 0), pltpu.roll(halo[c], SUB - 1, 0))
            near_flux = jnp.where(sub == 0, -pltpu.roll(flux[c], 1, 0), pltpu.roll(flux[c], SUB - 1, 0))
            end = jnp.logical_or(sub == 0, sub == SUB - 1)
            near = placed(jnp.where(end, near, nothing))
            near_flux = placed(jnp.where(end, near_flux, nothing))
            value = acc_f[c, x] - 0.5 * near_flux
            if c == 2:
                value = value + (0.5 * density) * placed(grad)
            value = step_all * (value + half_speed * (acc_l[c, x] + near))
            own = up[c, x + 1]
            fluid_out[c, x] = jnp.where(mask, own + value, own)
        return carry

    lax.fori_loop(0, nx, finish, 0)


def body(sizes, metric, curvature, conserved, matter_mask):
    shape = metric.shape[1:]
    nx, ny, nz = shape
    assert matter_mask.shape[:2] == (1, 1) and ny % SUB == 0 and ny >= 2 * SUB
    stages = stages_of(sizes)
    totals = [math.prod(sizes[axis] for axis in axes) for axes in stages]
    sides = 2 if sizes["gz"] > 2 else 1
    copies = 8 + 2 * sides
    vmem, sem = pltpu.VMEM, pltpu.SemaphoreType.DMA
    f32 = jnp.float32
    return pl.pallas_call(
        functools.partial(kernel, sizes, shape),
        out_shape=(
            jax.ShapeDtypeStruct((6,) + shape, f32),
            jax.ShapeDtypeStruct((6,) + shape, f32),
            jax.ShapeDtypeStruct((4,) + shape, f32),
        ),
        in_specs=[pl.BlockSpec(memory_space=pltpu.HBM)] * 4,
        out_specs=(pl.BlockSpec(memory_space=vmem),) * 3,
        scratch_shapes=[
            pltpu.SMEM(matter_mask.shape, jnp.int32),
            vmem((6, nx, ny, nz), f32),
            vmem((6, nx + 2 * W, ny, nz), f32),
            vmem((4, nx + 2, ny, nz), f32),
            vmem((sides, 6, nx, ny, nz), f32),
            vmem((sides, 4, nx, ny, nz), f32),
            vmem((6, nx, SUB, nz), f32),
            vmem((4, nx, SUB, nz), f32),
            vmem((6, nx, ny, nz), f32),
            vmem((4, nx, ny, nz), f32),
            vmem((4, nx, ny, nz), f32),
            vmem((len(stages), 1, nz), f32),
        ]
        + [vmem((total - 1, 1, nz), f32) for total in totals]
        + [sem((4,)), sem((copies,)), sem((copies,)), sem((len(stages),)), sem((len(stages),))],
        compiler_params=pltpu.CompilerParams(
            collective_id=0, has_side_effects=True, vmem_limit_bytes=24 * 1024 * 1024
        ),
        name="substep",
    )(metric, curvature, conserved, matter_mask)


def solution(mesh):
    sizes = {axis: mesh.shape[axis] for axis in AXES}
    grid = P(None, "gx", "gy", "gz")
    return jax.shard_map(
        functools.partial(body, sizes),
        mesh=mesh,
        in_specs=(grid, grid, grid, P("gx", "gy", "gz")),
        out_specs=(grid, grid, grid),
        check_vma=False,
    )
```

```python
import functools
import math

import jax
import jax.numpy as jnp
from jax import lax
from jax.experimental import pallas as pl
from jax.experimental.pallas import tpu as pltpu
from jax.sharding import PartitionSpec as P

MESH = pl.DeviceIdType.MESH
AXES = ("gx", "gy", "gz")
MB = 16
second = (-49.0 / 18.0, 1.5, -3.0 / 20.0, 1.0 / 90.0)
first = (0.0, 0.75, -3.0 / 20.0, 1.0 / 60.0)
sound_square = 0.25
sound_speed = 0.5
courant = 0.3
eight_pi = 8.0 * math.pi
pair_first = (0, 0, 0, 1, 1, 2)
pair_second = (0, 1, 2, 1, 2, 2)
trace_part = (0, 3, 5)
W = 3
SUB = 8


def peer(sizes, axes, offset):
    position = 0
    for axis in axes:
        position = position * sizes[axis] + lax.axis_index(axis)
    total = math.prod(sizes[axis] for axis in axes)
    position = lax.rem(position + offset, total)
    found = {}
    for axis in reversed(axes):
        found[axis] = lax.rem(position, sizes[axis])
        position = position // sizes[axis]
    return {axis: found.get(axis, lax.axis_index(axis)) for axis in AXES}


def stages_of(sizes):
    if math.prod(sizes.values()) <= 64:
        return (AXES,)
    return (("gz",), ("gy",), ("gx",))


def flux_of(state, direction):
    density, moment = state[0], state[1:]
    velocity = moment[direction] / density
    flux = [moment[direction]] + [moment[i] * velocity for i in range(3)]
    flux[1 + direction] = flux[1 + direction] + sound_square * density
    return flux


def kernel(sizes, shape, metric_hbm, curv_hbm, fluid_hbm, mask_hbm, metric_out, curv_out, fluid_out,
           mask_ref, cu, mp, up, ez, uz, ey, uy, acc_c, acc_f, acc_l, row, *rest):
    nx, ny, nz = shape
    stages = stages_of(sizes)
    bufs = rest[: len(stages)]
    load_sem, send_sem, recv_sem, row_send, row_recv = rest[len(stages):]
    tiles = ny // SUB

    own_m = mp.at[:, pl.ds(W, nx)]
    own_u = up.at[:, pl.ds(1, nx)]
    load_u = pltpu.make_async_copy(fluid_hbm, own_u, load_sem.at[0])
    load_m = pltpu.make_async_copy(metric_hbm, own_m, load_sem.at[1])
    load_mask = pltpu.make_async_copy(mask_hbm, mask_ref, load_sem.at[2])
    load_c = pltpu.make_async_copy(curv_hbm, cu, load_sem.at[3])
    load_mask.start()
    load_u.start()
    load_m.start()
    load_c.start()

    barrier = pltpu.get_barrier_semaphore()
    greeted = 0
    for axes in stages:
        total = math.prod(sizes[axis] for axis in axes)

        def greet(j, carry, axes=axes):
            pl.semaphore_signal(barrier, inc=1, device_id=peer(sizes, axes, j), device_id_type=MESH)
            return carry

        lax.fori_loop(1, total, greet, 0)
        greeted += total - 1

    load_mask.wait()
    lane = lax.broadcasted_iota(jnp.int32, (ny, nz), 1)
    block = lane // MB
    mask = jnp.zeros((ny, nz), jnp.int32)
    for b in range(nz // MB):
        mask = jnp.where(block == b, mask_ref[0, 0, b], mask)
    mask = mask > 0

    load_u.wait()

    def local_speed(x, best):
        moment = jnp.maximum(jnp.maximum(jnp.abs(up[1, x + 1]), jnp.abs(up[2, x + 1])), jnp.abs(up[3, x + 1]))
        speed = moment / up[0, x + 1] + sound_speed
        return jnp.maximum(best, jnp.where(mask, speed, jnp.float32(sound_speed)))

    best = lax.fori_loop(0, nx, local_speed, jnp.full((ny, nz), sound_speed, jnp.float32), unroll=4)
    best = jnp.max(best, axis=0, keepdims=True)
    row[0] = best
    load_m.wait()
    pl.semaphore_wait(barrier, greeted)

    def spread(index):
        axes = stages[index]
        total = math.prod(sizes[axis] for axis in axes)

        def send(j, carry):
            pltpu.make_async_remote_copy(
                src_ref=row.at[index], dst_ref=bufs[index].at[j - 1],
                send_sem=row_send.at[index], recv_sem=row_recv.at[index],
                device_id=peer(sizes, axes, j), device_id_type=MESH,
            ).start()
            return carry

        lax.fori_loop(1, total, send, 0)

    def gathered(index, best):
        buf = bufs[index]
        pltpu.make_async_copy(buf, buf, row_recv.at[index]).wait()
        pltpu.make_async_copy(buf, buf, row_send.at[index]).wait()
        return jnp.maximum(best, jnp.max(buf[...], axis=0))

    spread(0)

    count = [0]

    def remote(src, dst, axis, offset):
        n = count[0]
        count[0] += 1
        copy = pltpu.make_async_remote_copy(
            src_ref=src, dst_ref=dst, send_sem=send_sem.at[n], recv_sem=recv_sem.at[n],
            device_id=peer(sizes, (axis,), offset % sizes[axis]), device_id_type=MESH,
        )
        copy.start()
        return copy

    y_copies = [
        remote(mp.at[:, pl.ds(W, nx), pl.ds(ny - W, W)], ey.at[:, :, pl.ds(SUB - W, W)], "gy", 1),
        remote(mp.at[:, pl.ds(W, nx), pl.ds(0, W)], ey.at[:, :, pl.ds(0, W)], "gy", -1),
        remote(up.at[:, pl.ds(1, nx), pl.ds(ny - 1, 1)], uy.at[:, :, pl.ds(SUB - 1, 1)], "gy", 1),
        remote(up.at[:, pl.ds(1, nx), pl.ds(0, 1)], uy.at[:, :, pl.ds(0, 1)], "gy", -1),
    ]
    x_copies = [
        remote(mp.at[:, pl.ds(nx, W)], mp.at[:, pl.ds(0, W)], "gx", 1),
        remote(mp.at[:, pl.ds(W, W)], mp.at[:, pl.ds(nx + W, W)], "gx", -1),
        remote(up.at[:, pl.ds(nx, 1)], up.at[:, pl.ds(0, 1)], "gx", 1),
        remote(up.at[:, pl.ds(1, 1)], up.at[:, pl.ds(nx + 1, 1)], "gx", -1),
    ]
    z_copies = [remote(own_u, uz.at[0], "gz", -1), remote(own_m, ez.at[0], "gz", -1)]
    if sizes["gz"] > 2:
        z_copies += [remote(own_u, uz.at[1], "gz", 1), remote(own_m, ez.at[1], "gz", 1)]

    def edge(ref, c, x):
        if sizes["gz"] > 2:
            return jnp.where(lane < nz // 2, ref[0, c, x], ref[1, c, x])
        return ref[0, c, x]

    def z_up(own, other, k):
        return pltpu.roll(jnp.where(lane < k, other, own), nz - k, 1)

    def z_down(own, other, k):
        return pltpu.roll(jnp.where(lane >= nz - k, other, own), k, 1)

    sub = lax.broadcasted_iota(jnp.int32, (SUB, nz), 0)

    def cut(value):
        return [value[t * SUB : (t + 1) * SUB] for t in range(tiles)]

    def y_pair(value, k):
        own = cut(value)
        zero = jnp.zeros_like(own[0])
        after = own[1:] + [zero]
        before = [zero] + own[:-1]
        up_rows = [pltpu.roll(jnp.where(sub < k, after[t], own[t]), SUB - k, 0) for t in range(tiles)]
        down_rows = [pltpu.roll(jnp.where(sub >= SUB - k, before[t], own[t]), k, 0) for t in range(tiles)]
        return jnp.concatenate(up_rows, axis=0), jnp.concatenate(down_rows, axis=0)

    for copy in z_copies:
        copy.wait()

    def inner(x, carry):
        state = [up[c, x + 1] for c in range(4)]
        density, moment = state[0], state[1:]
        other = [edge(uz, c, x) for c in range(4)]
        above = [z_up(state[c], other[c], 1) for c in range(4)]
        below = [z_down(state[c], other[c], 1) for c in range(4)]
        flux_above, flux_below = flux_of(above, 2), flux_of(below, 2)
        flux_y = flux_of(state, 1)
        slopes = []
        for c in range(4):
            y_above, y_below = y_pair(state[c], 1)
            fy_above, fy_below = y_pair(flux_y[c], 1)
            slopes.append((flux_above[c] - flux_below[c]) + (fy_above - fy_below))
            acc_l[c, x] = (above[c] + below[c]) + (y_above + y_below) - 6.0 * state[c]
        grad_y = jnp.zeros((ny, nz), jnp.float32)
        grad_z = jnp.zeros((ny, nz), jnp.float32)
        inverse = 1.0 / density
        for c in range(6):
            own = mp[c, x + W]
            far = edge(ez, c, x)
            total = (3.0 * second[0]) * own
            for k in range(1, W + 1):
                zu, zd = z_up(own, far, k), z_down(own, far, k)
                yu, yd = y_pair(own, k)
                total = total + second[k] * ((zu + zd) + (yu + yd))
                if c in trace_part:
                    grad_z = grad_z + first[k] * (zu - zd)
                    grad_y = grad_y + first[k] * (yu - yd)
            stress = moment[pair_first[c]] * (moment[pair_second[c]] * inverse)
            if pair_first[c] == pair_second[c]:
                stress = stress + sound_square * density
            acc_c[c, x] = eight_pi * stress - 0.5 * total
        acc_f[0, x] = -0.5 * slopes[0]
        acc_f[1, x] = -0.5 * slopes[1]
        acc_f[2, x] = -0.5 * slopes[2] + (0.5 * density) * grad_y
        acc_f[3, x] = -0.5 * slopes[3] + (0.5 * density) * grad_z
        return carry

    lax.fori_loop(0, nx, inner, 0)

    for copy in x_copies:
        copy.wait()

    def along_x(x, carry):
        above = [up[c, x + 2] for c in range(4)]
        below = [up[c, x] for c in range(4)]
        flux_above, flux_below = flux_of(above, 0), flux_of(below, 0)
        grad = jnp.zeros((ny, nz), jnp.float32)
        for c in range(6):
            total = jnp.zeros((ny, nz), jnp.float32)
            for k in range(1, W + 1):
                high, low = mp[c, x + W + k], mp[c, x + W - k]
                total = total + second[k] * (high + low)
                if c in trace_part:
                    grad = grad + first[k] * (high - low)
            acc_c[c, x] = acc_c[c, x] - 0.5 * total
        for c in range(4):
            value = acc_f[c, x] - 0.5 * (flux_above[c] - flux_below[c])
            if c == 1:
                value = value + (0.5 * up[0, x + 1]) * grad
            acc_f[c, x] = value
            acc_l[c, x] = acc_l[c, x] + (above[c] + below[c])
        return carry

    lax.fori_loop(0, nx, along_x, 0)

    best = gathered(0, best)
    for index in range(1, len(stages)):
        row[index] = best
        spread(index)
        best = gathered(index, best)
    speed_max = jnp.max(best, axis=1, keepdims=True)
    step = courant / speed_max
    step_all = jnp.broadcast_to(step, (ny, nz))
    half_speed = jnp.broadcast_to(0.5 * speed_max, (ny, nz))

    load_c.wait()

    def advance_metric(x, carry):
        for c in range(6):
            metric_out[c, x] = mp[c, x + W] - (2.0 * step_all) * cu[c, x]
        return carry

    lax.fori_loop(0, nx, advance_metric, 0)

    for copy in y_copies:
        copy.wait()

    inside = jnp.logical_and(sub >= W, sub < SUB - W)
    weight, slope = [None], [None]
    for k in range(1, W + 1):
        touched = jnp.where(jnp.logical_or(sub < k, sub >= SUB - k), 1.0, 0.0)
        weight.append(touched * jnp.float32(second[k]))
        slope.append(jnp.where(sub < SUB // 2, -1.0, 1.0) * touched * jnp.float32(first[k]))
    low_half = sub < SUB // 2
    nothing = jnp.zeros((SUB, nz), jnp.float32)

    def placed(value):
        parts = [jnp.where(low_half, value, nothing)] + [nothing] * (tiles - 2) + [jnp.where(low_half, nothing, value)]
        return jnp.concatenate(parts, axis=0)

    def finish(x, carry):
        grad = nothing
        for c in range(6):
            halo = jnp.where(inside, nothing, ey[c, x])
            total = nothing
            for k in range(1, W + 1):
                near = jnp.where(low_half, pltpu.roll(halo, k, 0), pltpu.roll(halo, SUB - k, 0))
                total = total + weight[k] * near
                if c in trace_part:
                    grad = grad + slope[k] * near
            curv_out[c, x] = cu[c, x] + step_all * (acc_c[c, x] - 0.5 * placed(total))
        halo = [uy[c, x] for c in range(4)]
        flux = flux_of(halo, 1)
        density = up[0, x + 1]
        for c in range(4):
            near = jnp.where(sub == 0, pltpu.roll(halo[c], 1, 0), pltpu.roll(halo[c], SUB - 1, 0))
            near_flux = jnp.where(sub == 0, -pltpu.roll(flux[c], 1, 0), pltpu.roll(flux[c], SUB - 1, 0))
            end = jnp.logical_or(sub == 0, sub == SUB - 1)
            near = placed(jnp.where(end, near, nothing))
            near_flux = placed(jnp.where(end, near_flux, nothing))
            value = acc_f[c, x] - 0.5 * near_flux
            if c == 2:
                value = value + (0.5 * density) * placed(grad)
            value = step_all * (value + half_speed * (acc_l[c, x] + near))
            own = up[c, x + 1]
            fluid_out[c, x] = jnp.where(mask, own + value, own)
        return carry

    lax.fori_loop(0, nx, finish, 0)


def store(*refs):
    sems = refs[-1]
    copies = [pltpu.make_async_copy(refs[i], refs[3 + i], sems.at[i]) for i in range(3)]
    for copy in copies:
        copy.start()
    for copy in copies:
        copy.wait()


def body(sizes, metric, curvature, conserved, matter_mask):
    shape = metric.shape[1:]
    nx, ny, nz = shape
    assert matter_mask.shape[:2] == (1, 1) and ny % SUB == 0 and ny >= 2 * SUB
    stages = stages_of(sizes)
    totals = [math.prod(sizes[axis] for axis in axes) for axes in stages]
    sides = 2 if sizes["gz"] > 2 else 1
    copies = 8 + 2 * sides
    vmem, sem = pltpu.VMEM, pltpu.SemaphoreType.DMA
    f32 = jnp.float32
    metric, curvature, conserved, matter_mask = [
        pltpu.with_memory_space_constraint(x, pltpu.HBM) for x in (metric, curvature, conserved, matter_mask)
    ]
    parts = pl.pallas_call(
        functools.partial(kernel, sizes, shape),
        out_shape=(
            vmem((6,) + shape, f32),
            vmem((6,) + shape, f32),
            vmem((4,) + shape, f32),
        ),
        in_specs=[pl.BlockSpec(memory_space=pltpu.HBM)] * 4,
        out_specs=(pl.BlockSpec(memory_space=vmem),) * 3,
        scratch_shapes=[
            pltpu.SMEM(matter_mask.shape, jnp.int32),
            vmem((6, nx, ny, nz), f32),
            vmem((6, nx + 2 * W, ny, nz), f32),
            vmem((4, nx + 2, ny, nz), f32),
            vmem((sides, 6, nx, ny, nz), f32),
            vmem((sides, 4, nx, ny, nz), f32),
            vmem((6, nx, SUB, nz), f32),
            vmem((4, nx, SUB, nz), f32),
            vmem((6, nx, ny, nz), f32),
            vmem((4, nx, ny, nz), f32),
            vmem((4, nx, ny, nz), f32),
            vmem((len(stages), 1, nz), f32),
        ]
        + [vmem((total - 1, 1, nz), f32) for total in totals]
        + [sem((4,)), sem((copies,)), sem((copies,)), sem((len(stages),)), sem((len(stages),))],
        compiler_params=pltpu.CompilerParams(
            collective_id=0, has_side_effects=True, vmem_limit_bytes=24 * 1024 * 1024
        ),
        name="substep",
    )(metric, curvature, conserved, matter_mask)
    return pl.pallas_call(
        store,
        out_shape=tuple(jax.ShapeDtypeStruct(part.shape, f32) for part in parts),
        in_specs=[pl.BlockSpec(memory_space=vmem)] * 3,
        out_specs=(pl.BlockSpec(memory_space=pl.ANY),) * 3,
        scratch_shapes=[sem((3,))],
        compiler_params=pltpu.CompilerParams(vmem_limit_bytes=1024 * 1024),
        name="store",
    )(*parts)


def solution(mesh):
    sizes = {axis: mesh.shape[axis] for axis in AXES}
    grid = P(None, "gx", "gy", "gz")
    return jax.shard_map(
        functools.partial(body, sizes),
        mesh=mesh,
        in_specs=(grid, grid, grid, P("gx", "gy", "gz")),
        out_specs=(grid, grid, grid),
        check_vma=False,
    )
```

```python
import functools
import math

import jax
import jax.numpy as jnp
from jax import lax
from jax.experimental import pallas as pl
from jax.experimental.pallas import tpu as pltpu
from jax.sharding import PartitionSpec as P

MESH = pl.DeviceIdType.MESH
AXES = ("gx", "gy", "gz")
MB = 16
second = (-49.0 / 18.0, 1.5, -3.0 / 20.0, 1.0 / 90.0)
first = (0.0, 0.75, -3.0 / 20.0, 1.0 / 60.0)
sound_square = 0.25
sound_speed = 0.5
courant = 0.3
eight_pi = 8.0 * math.pi
pair_first = (0, 0, 0, 1, 1, 2)
pair_second = (0, 1, 2, 1, 2, 2)
trace_part = (0, 3, 5)
W = 3
SUB = 8


def peer(sizes, axes, offset):
    position = 0
    for axis in axes:
        position = position * sizes[axis] + lax.axis_index(axis)
    total = math.prod(sizes[axis] for axis in axes)
    position = lax.rem(position + offset, total)
    found = {}
    for axis in reversed(axes):
        found[axis] = lax.rem(position, sizes[axis])
        position = position // sizes[axis]
    return {axis: found.get(axis, lax.axis_index(axis)) for axis in AXES}


def stages_of(sizes):
    if math.prod(sizes.values()) <= 64:
        return (AXES,)
    return (("gz",), ("gy",), ("gx",))


def flux_of(state, direction):
    density, moment = state[0], state[1:]
    velocity = moment[direction] / density
    flux = [moment[direction]] + [moment[i] * velocity for i in range(3)]
    flux[1 + direction] = flux[1 + direction] + sound_square * density
    return flux


def kernel(sizes, shape, metric_hbm, curv_hbm, fluid_hbm, mask_hbm, metric_out, curv_out, fluid_out,
           mask_ref, cu, mp, up, ez, uz, ey, uy, acc_c, acc_f, acc_l, row, *rest):
    nx, ny, nz = shape
    stages = stages_of(sizes)
    bufs = rest[: len(stages)]
    load_sem, send_sem, recv_sem, row_send, row_recv = rest[len(stages):]
    tiles = ny // SUB

    own_m = mp.at[:, pl.ds(W, nx)]
    own_u = up.at[:, pl.ds(1, nx)]
    load_u = pltpu.make_async_copy(fluid_hbm, own_u, load_sem.at[0])
    load_m = pltpu.make_async_copy(metric_hbm, own_m, load_sem.at[1])
    load_mask = pltpu.make_async_copy(mask_hbm, mask_ref, load_sem.at[2])
    load_c = pltpu.make_async_copy(curv_hbm, cu, load_sem.at[3])
    barrier = pltpu.get_barrier_semaphore()
    greeted = 0
    for axes in stages:
        total = math.prod(sizes[axis] for axis in axes)

        def greet(j, carry, axes=axes):
            pl.semaphore_signal(barrier, inc=1, device_id=peer(sizes, axes, j), device_id_type=MESH)
            return carry

        lax.fori_loop(1, total, greet, 0)
        greeted += total - 1

    load_mask.start()
    load_u.start()
    load_m.start()
    load_c.start()

    load_mask.wait()
    lane = lax.broadcasted_iota(jnp.int32, (ny, nz), 1)
    block = lane // MB
    mask = jnp.zeros((ny, nz), jnp.int32)
    for b in range(nz // MB):
        mask = jnp.where(block == b, mask_ref[0, 0, b], mask)
    mask = mask > 0

    load_u.wait()

    def local_speed(x, best):
        moment = jnp.maximum(jnp.maximum(jnp.abs(up[1, x + 1]), jnp.abs(up[2, x + 1])), jnp.abs(up[3, x + 1]))
        speed = moment / up[0, x + 1] + sound_speed
        return jnp.maximum(best, jnp.where(mask, speed, jnp.float32(sound_speed)))

    best = lax.fori_loop(0, nx, local_speed, jnp.full((ny, nz), sound_speed, jnp.float32), unroll=4)
    best = jnp.max(best, axis=0, keepdims=True)
    row[0] = best
    load_m.wait()
    pl.semaphore_wait(barrier, greeted)

    def spread(index):
        axes = stages[index]
        total = math.prod(sizes[axis] for axis in axes)

        def send(j, carry):
            pltpu.make_async_remote_copy(
                src_ref=row.at[index], dst_ref=bufs[index].at[j - 1],
                send_sem=row_send.at[index], recv_sem=row_recv.at[index],
                device_id=peer(sizes, axes, j), device_id_type=MESH,
            ).start()
            return carry

        lax.fori_loop(1, total, send, 0)

    def gathered(index, best):
        buf = bufs[index]
        pltpu.make_async_copy(buf, buf, row_recv.at[index]).wait()
        pltpu.make_async_copy(buf, buf, row_send.at[index]).wait()
        return jnp.maximum(best, jnp.max(buf[...], axis=0))

    count = [0]

    def remote(src, dst, axis, offset):
        n = count[0]
        count[0] += 1
        copy = pltpu.make_async_remote_copy(
            src_ref=src, dst_ref=dst, send_sem=send_sem.at[n], recv_sem=recv_sem.at[n],
            device_id=peer(sizes, (axis,), offset % sizes[axis]), device_id_type=MESH,
        )
        copy.start()
        return copy

    z_copies = [remote(own_u, uz.at[0], "gz", -1), remote(own_m, ez.at[0], "gz", -1)]
    if sizes["gz"] > 2:
        z_copies += [remote(own_u, uz.at[1], "gz", 1), remote(own_m, ez.at[1], "gz", 1)]

    def metric_sides(start):
        some = pl.ds(start, 3)
        return [
            remote(mp.at[some, pl.ds(W, nx), pl.ds(ny - W, W)], ey.at[some, :, pl.ds(SUB - W, W)], "gy", 1),
            remote(mp.at[some, pl.ds(W, nx), pl.ds(0, W)], ey.at[some, :, pl.ds(0, W)], "gy", -1),
            remote(mp.at[some, pl.ds(nx, W)], mp.at[some, pl.ds(0, W)], "gx", 1),
            remote(mp.at[some, pl.ds(W, W)], mp.at[some, pl.ds(nx + W, W)], "gx", -1),
        ]

    early = [
        remote(up.at[:, pl.ds(1, nx), pl.ds(ny - 1, 1)], uy.at[:, :, pl.ds(SUB - 1, 1)], "gy", 1),
        remote(up.at[:, pl.ds(1, nx), pl.ds(0, 1)], uy.at[:, :, pl.ds(0, 1)], "gy", -1),
        remote(up.at[:, pl.ds(nx, 1)], up.at[:, pl.ds(0, 1)], "gx", 1),
        remote(up.at[:, pl.ds(1, 1)], up.at[:, pl.ds(nx + 1, 1)], "gx", -1),
    ] + metric_sides(0)
    spread(0)
    late = metric_sides(3)

    def edge(ref, c, x):
        if sizes["gz"] > 2:
            return jnp.where(lane < nz // 2, ref[0, c, x], ref[1, c, x])
        return ref[0, c, x]

    def z_up(own, other, k):
        return pltpu.roll(jnp.where(lane < k, other, own), nz - k, 1)

    def z_down(own, other, k):
        return pltpu.roll(jnp.where(lane >= nz - k, other, own), k, 1)

    sub = lax.broadcasted_iota(jnp.int32, (SUB, nz), 0)

    def cut(value):
        return [value[t * SUB : (t + 1) * SUB] for t in range(tiles)]

    def y_pair(value, k):
        own = cut(value)
        zero = jnp.zeros_like(own[0])
        after = own[1:] + [zero]
        before = [zero] + own[:-1]
        up_rows = [pltpu.roll(jnp.where(sub < k, after[t], own[t]), SUB - k, 0) for t in range(tiles)]
        down_rows = [pltpu.roll(jnp.where(sub >= SUB - k, before[t], own[t]), k, 0) for t in range(tiles)]
        return jnp.concatenate(up_rows, axis=0), jnp.concatenate(down_rows, axis=0)

    for copy in z_copies:
        copy.wait()

    def inner(x, carry):
        state = [up[c, x + 1] for c in range(4)]
        density, moment = state[0], state[1:]
        other = [edge(uz, c, x) for c in range(4)]
        above = [z_up(state[c], other[c], 1) for c in range(4)]
        below = [z_down(state[c], other[c], 1) for c in range(4)]
        flux_above, flux_below = flux_of(above, 2), flux_of(below, 2)
        flux_y = flux_of(state, 1)
        slopes = []
        for c in range(4):
            y_above, y_below = y_pair(state[c], 1)
            fy_above, fy_below = y_pair(flux_y[c], 1)
            slopes.append((flux_above[c] - flux_below[c]) + (fy_above - fy_below))
            acc_l[c, x] = (above[c] + below[c]) + (y_above + y_below) - 6.0 * state[c]
        grad_y = jnp.zeros((ny, nz), jnp.float32)
        grad_z = jnp.zeros((ny, nz), jnp.float32)
        inverse = 1.0 / density
        for c in range(6):
            own = mp[c, x + W]
            far = edge(ez, c, x)
            total = (3.0 * second[0]) * own
            for k in range(1, W + 1):
                zu, zd = z_up(own, far, k), z_down(own, far, k)
                yu, yd = y_pair(own, k)
                total = total + second[k] * ((zu + zd) + (yu + yd))
                if c in trace_part:
                    grad_z = grad_z + first[k] * (zu - zd)
                    grad_y = grad_y + first[k] * (yu - yd)
            stress = moment[pair_first[c]] * (moment[pair_second[c]] * inverse)
            if pair_first[c] == pair_second[c]:
                stress = stress + sound_square * density
            acc_c[c, x] = eight_pi * stress - 0.5 * total
        acc_f[0, x] = -0.5 * slopes[0]
        acc_f[1, x] = -0.5 * slopes[1]
        acc_f[2, x] = -0.5 * slopes[2] + (0.5 * density) * grad_y
        acc_f[3, x] = -0.5 * slopes[3] + (0.5 * density) * grad_z
        return carry

    lax.fori_loop(0, nx, inner, 0)

    inside = jnp.logical_and(sub >= W, sub < SUB - W)
    weight, slope = [None], [None]
    for k in range(1, W + 1):
        touched = jnp.where(jnp.logical_or(sub < k, sub >= SUB - k), 1.0, 0.0)
        weight.append(touched * jnp.float32(second[k]))
        slope.append(jnp.where(sub < SUB // 2, -1.0, 1.0) * touched * jnp.float32(first[k]))
    low_half = sub < SUB // 2
    nothing = jnp.zeros((SUB, nz), jnp.float32)

    def placed(value):
        parts = [jnp.where(low_half, value, nothing)] + [nothing] * (tiles - 2) + [jnp.where(low_half, nothing, value)]
        return jnp.concatenate(parts, axis=0)

    def sides(c, x):
        total = jnp.zeros((ny, nz), jnp.float32)
        grad_x = jnp.zeros((ny, nz), jnp.float32)
        halo = jnp.where(inside, nothing, ey[c, x])
        rows, grad_y = nothing, nothing
        for k in range(1, W + 1):
            high, low = mp[c, x + W + k], mp[c, x + W - k]
            near = jnp.where(low_half, pltpu.roll(halo, k, 0), pltpu.roll(halo, SUB - k, 0))
            total = total + second[k] * (high + low)
            rows = rows + weight[k] * near
            grad_x = grad_x + first[k] * (high - low)
            grad_y = grad_y + slope[k] * near
        return total + placed(rows), grad_x, grad_y

    for copy in early:
        copy.wait()

    def first_half(x, carry):
        for c in range(3):
            total, grad_x, grad_y = sides(c, x)
            acc_c[c, x] = acc_c[c, x] - 0.5 * total
            if c == 0:
                gx, gy = grad_x, placed(grad_y)
        half_density = 0.5 * up[0, x + 1]
        above = [up[c, x + 2] for c in range(4)]
        below = [up[c, x] for c in range(4)]
        flux_above, flux_below = flux_of(above, 0), flux_of(below, 0)
        halo = [uy[c, x] for c in range(4)]
        flux = flux_of(halo, 1)
        end = jnp.logical_or(sub == 0, sub == SUB - 1)
        for c in range(4):
            near = jnp.where(sub == 0, pltpu.roll(halo[c], 1, 0), pltpu.roll(halo[c], SUB - 1, 0))
            near_flux = jnp.where(sub == 0, -pltpu.roll(flux[c], 1, 0), pltpu.roll(flux[c], SUB - 1, 0))
            near = placed(jnp.where(end, near, nothing))
            near_flux = placed(jnp.where(end, near_flux, nothing))
            value = acc_f[c, x] - 0.5 * ((flux_above[c] - flux_below[c]) + near_flux)
            if c == 1:
                value = value + half_density * gx
            if c == 2:
                value = value + half_density * gy
            acc_f[c, x] = value
            acc_l[c, x] = acc_l[c, x] + ((above[c] + below[c]) + near)
        return carry

    lax.fori_loop(0, nx, first_half, 0)

    best = gathered(0, best)
    for index in range(1, len(stages)):
        row[index] = best
        spread(index)
        best = gathered(index, best)
    speed_max = jnp.max(best, axis=1, keepdims=True)
    step = courant / speed_max
    step_all = jnp.broadcast_to(step, (ny, nz))
    half_speed = jnp.broadcast_to(0.5 * speed_max, (ny, nz))

    load_c.wait()

    def advance(x, carry):
        for c in range(6):
            metric_out[c, x] = mp[c, x + W] - (2.0 * step_all) * cu[c, x]
        for c in range(3):
            curv_out[c, x] = cu[c, x] + step_all * acc_c[c, x]
        own = [up[c, x + 1] for c in range(4)]
        for c in (0, 3):
            add = acc_f[c, x] + half_speed * acc_l[c, x]
            fluid_out[c, x] = jnp.where(mask, own[c] + step_all * add, own[c])
        return carry

    lax.fori_loop(0, nx, advance, 0)

    for copy in late:
        copy.wait()

    def second_half(x, carry):
        gx = jnp.zeros((ny, nz), jnp.float32)
        gy = nothing
        for c in range(3, 6):
            total, grad_x, grad_y = sides(c, x)
            curv_out[c, x] = cu[c, x] + step_all * (acc_c[c, x] - 0.5 * total)
            if c in trace_part:
                gx, gy = gx + grad_x, gy + grad_y
        half_density = 0.5 * up[0, x + 1]
        for c, grad in ((1, gx), (2, placed(gy))):
            own = up[c, x + 1]
            add = acc_f[c, x] + half_density * grad + half_speed * acc_l[c, x]
            fluid_out[c, x] = jnp.where(mask, own + step_all * add, own)
        return carry

    lax.fori_loop(0, nx, second_half, 0)


def store(*refs):
    sems = refs[-1]
    copies = [pltpu.make_async_copy(refs[i], refs[3 + i], sems.at[i]) for i in range(3)]
    for copy in copies:
        copy.start()
    for copy in copies:
        copy.wait()


def body(sizes, metric, curvature, conserved, matter_mask):
    shape = metric.shape[1:]
    nx, ny, nz = shape
    assert matter_mask.shape[:2] == (1, 1) and ny % SUB == 0 and ny >= 2 * SUB
    stages = stages_of(sizes)
    totals = [math.prod(sizes[axis] for axis in axes) for axes in stages]
    sides = 2 if sizes["gz"] > 2 else 1
    copies = 12 + 2 * sides
    vmem, sem = pltpu.VMEM, pltpu.SemaphoreType.DMA
    f32 = jnp.float32
    metric, curvature, conserved, matter_mask = [
        pltpu.with_memory_space_constraint(x, pltpu.HBM) for x in (metric, curvature, conserved, matter_mask)
    ]
    parts = pl.pallas_call(
        functools.partial(kernel, sizes, shape),
        out_shape=(
            vmem((6,) + shape, f32),
            vmem((6,) + shape, f32),
            vmem((4,) + shape, f32),
        ),
        in_specs=[pl.BlockSpec(memory_space=pltpu.HBM)] * 4,
        out_specs=(pl.BlockSpec(memory_space=vmem),) * 3,
        scratch_shapes=[
            pltpu.SMEM(matter_mask.shape, jnp.int32),
            vmem((6, nx, ny, nz), f32),
            vmem((6, nx + 2 * W, ny, nz), f32),
            vmem((4, nx + 2, ny, nz), f32),
            vmem((sides, 6, nx, ny, nz), f32),
            vmem((sides, 4, nx, ny, nz), f32),
            vmem((6, nx, SUB, nz), f32),
            vmem((4, nx, SUB, nz), f32),
            vmem((6, nx, ny, nz), f32),
            vmem((4, nx, ny, nz), f32),
            vmem((4, nx, ny, nz), f32),
            vmem((len(stages), 1, nz), f32),
        ]
        + [vmem((total - 1, 1, nz), f32) for total in totals]
        + [sem((4,)), sem((copies,)), sem((copies,)), sem((len(stages),)), sem((len(stages),))],
        compiler_params=pltpu.CompilerParams(
            collective_id=0, has_side_effects=True, vmem_limit_bytes=24 * 1024 * 1024
        ),
        name="substep",
    )(metric, curvature, conserved, matter_mask)
    return pl.pallas_call(
        store,
        out_shape=tuple(jax.ShapeDtypeStruct(part.shape, f32) for part in parts),
        in_specs=[pl.BlockSpec(memory_space=vmem)] * 3,
        out_specs=(pl.BlockSpec(memory_space=pl.ANY),) * 3,
        scratch_shapes=[sem((3,))],
        compiler_params=pltpu.CompilerParams(vmem_limit_bytes=1024 * 1024),
        name="store",
    )(*parts)


def solution(mesh):
    sizes = {axis: mesh.shape[axis] for axis in AXES}
    grid = P(None, "gx", "gy", "gz")
    return jax.shard_map(
        functools.partial(body, sizes),
        mesh=mesh,
        in_specs=(grid, grid, grid, P("gx", "gy", "gz")),
        out_specs=(grid, grid, grid),
        check_vma=False,
    )
```

```python
import functools
import math

import jax
import jax.numpy as jnp
from jax import lax
from jax.experimental import pallas as pl
from jax.experimental.pallas import tpu as pltpu
from jax.sharding import PartitionSpec as P

MESH = pl.DeviceIdType.MESH
AXES = ("gx", "gy", "gz")
MB = 16
second = (-49.0 / 18.0, 1.5, -3.0 / 20.0, 1.0 / 90.0)
first = (0.0, 0.75, -3.0 / 20.0, 1.0 / 60.0)
sound_square = 0.25
sound_speed = 0.5
courant = 0.3
eight_pi = 8.0 * math.pi
pair_first = (0, 0, 0, 1, 1, 2)
pair_second = (0, 1, 2, 1, 2, 2)
trace_part = (0, 3, 5)
W = 3
SUB = 8
EARLY = 4


def peer(sizes, axes, offset):
    position = 0
    for axis in axes:
        position = position * sizes[axis] + lax.axis_index(axis)
    total = math.prod(sizes[axis] for axis in axes)
    position = lax.rem(position + offset, total)
    found = {}
    for axis in reversed(axes):
        found[axis] = lax.rem(position, sizes[axis])
        position = position // sizes[axis]
    return {axis: found.get(axis, lax.axis_index(axis)) for axis in AXES}


def stages_of(sizes):
    if math.prod(sizes.values()) <= 64:
        return (AXES,)
    return (("gz",), ("gy",), ("gx",))


def flux_of(state, direction):
    density, moment = state[0], state[1:]
    velocity = moment[direction] / density
    flux = [moment[direction]] + [moment[i] * velocity for i in range(3)]
    flux[1 + direction] = flux[1 + direction] + sound_square * density
    return flux


def kernel(sizes, shape, metric_hbm, curv_hbm, fluid_hbm, mask_hbm, metric_out, curv_out, fluid_out,
           mask_ref, cu, mp, up, ez, uz, ey, uy, acc_c, acc_f, acc_l, row, *rest):
    nx, ny, nz = shape
    stages = stages_of(sizes)
    bufs = rest[: len(stages)]
    load_sem, send_sem, recv_sem, row_send, row_recv = rest[len(stages):]
    tiles = ny // SUB

    own_m = mp.at[:, pl.ds(W, nx)]
    own_u = up.at[:, pl.ds(1, nx)]
    load_u = pltpu.make_async_copy(fluid_hbm, own_u, load_sem.at[0])
    load_m = pltpu.make_async_copy(metric_hbm, own_m, load_sem.at[1])
    load_mask = pltpu.make_async_copy(mask_hbm, mask_ref, load_sem.at[2])
    load_c = pltpu.make_async_copy(curv_hbm, cu, load_sem.at[3])
    barrier = pltpu.get_barrier_semaphore()
    greeted = 0
    for axes in stages:
        total = math.prod(sizes[axis] for axis in axes)

        def greet(j, carry, axes=axes):
            pl.semaphore_signal(barrier, inc=1, device_id=peer(sizes, axes, j), device_id_type=MESH)
            return carry

        lax.fori_loop(1, total, greet, 0)
        greeted += total - 1

    load_mask.start()
    load_u.start()
    load_m.start()
    load_c.start()

    load_mask.wait()
    lane = lax.broadcasted_iota(jnp.int32, (ny, nz), 1)
    block = lane // MB
    mask = jnp.zeros((ny, nz), jnp.int32)
    for b in range(nz // MB):
        mask = jnp.where(block == b, mask_ref[0, 0, b], mask)
    mask = mask > 0

    load_u.wait()

    def local_speed(x, best):
        moment = jnp.maximum(jnp.maximum(jnp.abs(up[1, x + 1]), jnp.abs(up[2, x + 1])), jnp.abs(up[3, x + 1]))
        speed = moment / up[0, x + 1] + sound_speed
        return jnp.maximum(best, jnp.where(mask, speed, jnp.float32(sound_speed)))

    best = lax.fori_loop(0, nx, local_speed, jnp.full((ny, nz), sound_speed, jnp.float32), unroll=4)
    best = jnp.max(best, axis=0, keepdims=True)
    row[0] = best
    load_m.wait()
    pl.semaphore_wait(barrier, greeted)

    def spread(index):
        axes = stages[index]
        total = math.prod(sizes[axis] for axis in axes)

        def send(j, carry):
            pltpu.make_async_remote_copy(
                src_ref=row.at[index], dst_ref=bufs[index].at[j - 1],
                send_sem=row_send.at[index], recv_sem=row_recv.at[index],
                device_id=peer(sizes, axes, j), device_id_type=MESH,
            ).start()
            return carry

        lax.fori_loop(1, total, send, 0)

    def gathered(index, best):
        buf = bufs[index]
        pltpu.make_async_copy(buf, buf, row_recv.at[index]).wait()
        pltpu.make_async_copy(buf, buf, row_send.at[index]).wait()
        return jnp.maximum(best, jnp.max(buf[...], axis=0))

    count = [0]

    def remote(src, dst, axis, offset):
        n = count[0]
        count[0] += 1
        copy = pltpu.make_async_remote_copy(
            src_ref=src, dst_ref=dst, send_sem=send_sem.at[n], recv_sem=recv_sem.at[n],
            device_id=peer(sizes, (axis,), offset % sizes[axis]), device_id_type=MESH,
        )
        copy.start()
        return copy

    z_copies = [remote(own_u, uz.at[0], "gz", -1), remote(own_m, ez.at[0], "gz", -1)]
    if sizes["gz"] > 2:
        z_copies += [remote(own_u, uz.at[1], "gz", 1), remote(own_m, ez.at[1], "gz", 1)]

    def metric_sides(start, stop):
        some = pl.ds(start, stop - start)
        return [
            remote(mp.at[some, pl.ds(W, nx), pl.ds(ny - W, W)], ey.at[some, :, pl.ds(SUB - W, W)], "gy", 1),
            remote(mp.at[some, pl.ds(W, nx), pl.ds(0, W)], ey.at[some, :, pl.ds(0, W)], "gy", -1),
            remote(mp.at[some, pl.ds(nx, W)], mp.at[some, pl.ds(0, W)], "gx", 1),
            remote(mp.at[some, pl.ds(W, W)], mp.at[some, pl.ds(nx + W, W)], "gx", -1),
        ]

    early = [
        remote(up.at[:, pl.ds(1, nx), pl.ds(ny - 1, 1)], uy.at[:, :, pl.ds(SUB - 1, 1)], "gy", 1),
        remote(up.at[:, pl.ds(1, nx), pl.ds(0, 1)], uy.at[:, :, pl.ds(0, 1)], "gy", -1),
        remote(up.at[:, pl.ds(nx, 1)], up.at[:, pl.ds(0, 1)], "gx", 1),
        remote(up.at[:, pl.ds(1, 1)], up.at[:, pl.ds(nx + 1, 1)], "gx", -1),
    ] + metric_sides(0, EARLY)
    spread(0)
    late = metric_sides(EARLY, 6)

    def edge(ref, c, x):
        if sizes["gz"] > 2:
            return jnp.where(lane < nz // 2, ref[0, c, x], ref[1, c, x])
        return ref[0, c, x]

    def z_up(own, other, k):
        return pltpu.roll(jnp.where(lane < k, other, own), nz - k, 1)

    def z_down(own, other, k):
        return pltpu.roll(jnp.where(lane >= nz - k, other, own), k, 1)

    sub = lax.broadcasted_iota(jnp.int32, (SUB, nz), 0)

    def cut(value):
        return [value[t * SUB : (t + 1) * SUB] for t in range(tiles)]

    def y_pair(value, k):
        own = cut(value)
        zero = jnp.zeros_like(own[0])
        after = own[1:] + [zero]
        before = [zero] + own[:-1]
        up_rows = [pltpu.roll(jnp.where(sub < k, after[t], own[t]), SUB - k, 0) for t in range(tiles)]
        down_rows = [pltpu.roll(jnp.where(sub >= SUB - k, before[t], own[t]), k, 0) for t in range(tiles)]
        return jnp.concatenate(up_rows, axis=0), jnp.concatenate(down_rows, axis=0)

    for copy in z_copies:
        copy.wait()

    def inner(x, carry):
        state = [up[c, x + 1] for c in range(4)]
        density, moment = state[0], state[1:]
        other = [edge(uz, c, x) for c in range(4)]
        above = [z_up(state[c], other[c], 1) for c in range(4)]
        below = [z_down(state[c], other[c], 1) for c in range(4)]
        flux_above, flux_below = flux_of(above, 2), flux_of(below, 2)
        flux_y = flux_of(state, 1)
        slopes = []
        for c in range(4):
            y_above, y_below = y_pair(state[c], 1)
            fy_above, fy_below = y_pair(flux_y[c], 1)
            slopes.append((flux_above[c] - flux_below[c]) + (fy_above - fy_below))
            acc_l[c, x] = (above[c] + below[c]) + (y_above + y_below) - 6.0 * state[c]
        grad_y = jnp.zeros((ny, nz), jnp.float32)
        grad_z = jnp.zeros((ny, nz), jnp.float32)
        inverse = 1.0 / density
        for c in range(6):
            own = mp[c, x + W]
            far = edge(ez, c, x)
            total = (3.0 * second[0]) * own
            for k in range(1, W + 1):
                zu, zd = z_up(own, far, k), z_down(own, far, k)
                yu, yd = y_pair(own, k)
                total = total + second[k] * ((zu + zd) + (yu + yd))
                if c in trace_part:
                    grad_z = grad_z + first[k] * (zu - zd)
                    grad_y = grad_y + first[k] * (yu - yd)
            stress = moment[pair_first[c]] * (moment[pair_second[c]] * inverse)
            if pair_first[c] == pair_second[c]:
                stress = stress + sound_square * density
            acc_c[c, x] = eight_pi * stress - 0.5 * total
        acc_f[0, x] = -0.5 * slopes[0]
        acc_f[1, x] = -0.5 * slopes[1]
        acc_f[2, x] = -0.5 * slopes[2] + (0.5 * density) * grad_y
        acc_f[3, x] = -0.5 * slopes[3] + (0.5 * density) * grad_z
        return carry

    lax.fori_loop(0, nx, inner, 0)

    inside = jnp.logical_and(sub >= W, sub < SUB - W)
    weight, slope = [None], [None]
    for k in range(1, W + 1):
        touched = jnp.where(jnp.logical_or(sub < k, sub >= SUB - k), 1.0, 0.0)
        weight.append(touched * jnp.float32(second[k]))
        slope.append(jnp.where(sub < SUB // 2, -1.0, 1.0) * touched * jnp.float32(first[k]))
    low_half = sub < SUB // 2
    nothing = jnp.zeros((SUB, nz), jnp.float32)

    def placed(value):
        parts = [jnp.where(low_half, value, nothing)] + [nothing] * (tiles - 2) + [jnp.where(low_half, nothing, value)]
        return jnp.concatenate(parts, axis=0)

    def sides(c, x):
        total = jnp.zeros((ny, nz), jnp.float32)
        grad_x = jnp.zeros((ny, nz), jnp.float32)
        halo = jnp.where(inside, nothing, ey[c, x])
        rows, grad_y = nothing, nothing
        for k in range(1, W + 1):
            high, low = mp[c, x + W + k], mp[c, x + W - k]
            near = jnp.where(low_half, pltpu.roll(halo, k, 0), pltpu.roll(halo, SUB - k, 0))
            total = total + second[k] * (high + low)
            rows = rows + weight[k] * near
            grad_x = grad_x + first[k] * (high - low)
            grad_y = grad_y + slope[k] * near
        return total + placed(rows), grad_x, grad_y

    for copy in early:
        copy.wait()

    def first_half(x, carry):
        gx, gy = jnp.zeros((ny, nz), jnp.float32), nothing
        for c in range(EARLY):
            total, grad_x, grad_y = sides(c, x)
            acc_c[c, x] = acc_c[c, x] - 0.5 * total
            if c in trace_part:
                gx, gy = gx + grad_x, gy + grad_y
        gy = placed(gy)
        half_density = 0.5 * up[0, x + 1]
        above = [up[c, x + 2] for c in range(4)]
        below = [up[c, x] for c in range(4)]
        flux_above, flux_below = flux_of(above, 0), flux_of(below, 0)
        halo = [uy[c, x] for c in range(4)]
        flux = flux_of(halo, 1)
        end = jnp.logical_or(sub == 0, sub == SUB - 1)
        for c in range(4):
            near = jnp.where(sub == 0, pltpu.roll(halo[c], 1, 0), pltpu.roll(halo[c], SUB - 1, 0))
            near_flux = jnp.where(sub == 0, -pltpu.roll(flux[c], 1, 0), pltpu.roll(flux[c], SUB - 1, 0))
            near = placed(jnp.where(end, near, nothing))
            near_flux = placed(jnp.where(end, near_flux, nothing))
            value = acc_f[c, x] - 0.5 * ((flux_above[c] - flux_below[c]) + near_flux)
            if c == 1:
                value = value + half_density * gx
            if c == 2:
                value = value + half_density * gy
            acc_f[c, x] = value
            acc_l[c, x] = acc_l[c, x] + ((above[c] + below[c]) + near)
        return carry

    lax.fori_loop(0, nx, first_half, 0)

    best = gathered(0, best)
    for index in range(1, len(stages)):
        row[index] = best
        spread(index)
        best = gathered(index, best)
    speed_max = jnp.max(best, axis=1, keepdims=True)
    step = courant / speed_max
    step_all = jnp.broadcast_to(step, (ny, nz))
    half_speed = jnp.broadcast_to(0.5 * speed_max, (ny, nz))

    load_c.wait()

    def advance(x, carry):
        for c in range(6):
            metric_out[c, x] = mp[c, x + W] - (2.0 * step_all) * cu[c, x]
        for c in range(EARLY):
            curv_out[c, x] = cu[c, x] + step_all * acc_c[c, x]
        own = [up[c, x + 1] for c in range(4)]
        for c in (0, 3):
            add = acc_f[c, x] + half_speed * acc_l[c, x]
            fluid_out[c, x] = jnp.where(mask, own[c] + step_all * add, own[c])
        return carry

    lax.fori_loop(0, nx, advance, 0)

    for copy in late:
        copy.wait()

    def second_half(x, carry):
        gx = jnp.zeros((ny, nz), jnp.float32)
        gy = nothing
        for c in range(EARLY, 6):
            total, grad_x, grad_y = sides(c, x)
            curv_out[c, x] = cu[c, x] + step_all * (acc_c[c, x] - 0.5 * total)
            if c in trace_part:
                gx, gy = gx + grad_x, gy + grad_y
        half_density = 0.5 * up[0, x + 1]
        for c, grad in ((1, gx), (2, placed(gy))):
            own = up[c, x + 1]
            add = acc_f[c, x] + half_density * grad + half_speed * acc_l[c, x]
            fluid_out[c, x] = jnp.where(mask, own + step_all * add, own)
        return carry

    lax.fori_loop(0, nx, second_half, 0, unroll=2)


def store(*refs):
    sems = refs[-1]
    copies = [pltpu.make_async_copy(refs[i], refs[3 + i], sems.at[i]) for i in range(3)]
    for copy in copies:
        copy.start()
    for copy in copies:
        copy.wait()


def body(sizes, metric, curvature, conserved, matter_mask):
    shape = metric.shape[1:]
    nx, ny, nz = shape
    assert matter_mask.shape[:2] == (1, 1) and ny % SUB == 0 and ny >= 2 * SUB
    stages = stages_of(sizes)
    totals = [math.prod(sizes[axis] for axis in axes) for axes in stages]
    sides = 2 if sizes["gz"] > 2 else 1
    copies = 12 + 2 * sides
    vmem, sem = pltpu.VMEM, pltpu.SemaphoreType.DMA
    f32 = jnp.float32
    metric, curvature, conserved, matter_mask = [
        pltpu.with_memory_space_constraint(x, pltpu.HBM) for x in (metric, curvature, conserved, matter_mask)
    ]
    parts = pl.pallas_call(
        functools.partial(kernel, sizes, shape),
        out_shape=(
            vmem((6,) + shape, f32),
            vmem((6,) + shape, f32),
            vmem((4,) + shape, f32),
        ),
        in_specs=[pl.BlockSpec(memory_space=pltpu.HBM)] * 4,
        out_specs=(pl.BlockSpec(memory_space=vmem),) * 3,
        scratch_shapes=[
            pltpu.SMEM(matter_mask.shape, jnp.int32),
            vmem((6, nx, ny, nz), f32),
            vmem((6, nx + 2 * W, ny, nz), f32),
            vmem((4, nx + 2, ny, nz), f32),
            vmem((sides, 6, nx, ny, nz), f32),
            vmem((sides, 4, nx, ny, nz), f32),
            vmem((6, nx, SUB, nz), f32),
            vmem((4, nx, SUB, nz), f32),
            vmem((6, nx, ny, nz), f32),
            vmem((4, nx, ny, nz), f32),
            vmem((4, nx, ny, nz), f32),
            vmem((len(stages), 1, nz), f32),
        ]
        + [vmem((total - 1, 1, nz), f32) for total in totals]
        + [sem((4,)), sem((copies,)), sem((copies,)), sem((len(stages),)), sem((len(stages),))],
        compiler_params=pltpu.CompilerParams(
            collective_id=0, has_side_effects=True, vmem_limit_bytes=24 * 1024 * 1024
        ),
        name="substep",
    )(metric, curvature, conserved, matter_mask)
    return pl.pallas_call(
        store,
        out_shape=tuple(jax.ShapeDtypeStruct(part.shape, f32) for part in parts),
        in_specs=[pl.BlockSpec(memory_space=vmem)] * 3,
        out_specs=(pl.BlockSpec(memory_space=pl.ANY),) * 3,
        scratch_shapes=[sem((3,))],
        compiler_params=pltpu.CompilerParams(vmem_limit_bytes=1024 * 1024),
        name="store",
    )(*parts)


def solution(mesh):
    sizes = {axis: mesh.shape[axis] for axis in AXES}
    grid = P(None, "gx", "gy", "gz")
    return jax.shard_map(
        functools.partial(body, sizes),
        mesh=mesh,
        in_specs=(grid, grid, grid, P("gx", "gy", "gz")),
        out_specs=(grid, grid, grid),
        check_vma=False,
    )
```
